32 devices in a mesh: shard: 4 (over z), context: 2 (over x), tensor: 4 (over y, core).
Axes of the slice: x: 2, y: 2, z: 4, core: 2. Of those that a mesh axis runs over, the one named last changes fastest.
Arguments:
- x_data: bfloat16 [4, 4, 2, 256, 2048], P(None, 'shard', 'context'), may hold values from -6 to 6
- cotangent: bfloat16 [4, 4, 2, 256, 2048], P('shard', None, 'context'), may hold values from -6 to 6
- lengths: int32 [4], replicated, may hold values from 1024 to 2048, as said below
- order: int32 [4], replicated, may hold values from 0 to 3, each once
- query_weight: float32 [2048, 2048], P(('shard', 'context'), 'tensor'), may hold values from -0.1875 to 0.1875
- key_weight: float32 [2048, 2048], P(('shard', 'context'), 'tensor'), may hold values from -0.1875 to 0.1875
- value_weight: float32 [2048, 2048], P(('shard', 'context'), 'tensor'), may hold values from -0.125 to 0.125
- out_weight: float32 [2048, 2048], P('tensor', ('shard', 'context')), may hold values from -0.5 to 0.5
- gate_weight: float32 [2048, 8192], P(('shard', 'context'), 'tensor'), may hold values from -0.125 to 0.125
- up_weight: float32 [2048, 8192], P(('shard', 'context'), 'tensor'), may hold values from -0.125 to 0.125
- down_weight: float32 [8192, 2048], P('tensor', ('shard', 'context')), may hold values from -0.0625 to 0.0625
- query_moment: float32 [2048, 2048], P(('shard', 'context'), 'tensor'), may hold values from -896 to 896
- key_moment: float32 [2048, 2048], P(('shard', 'context'), 'tensor'), may hold values from -896 to 896
- value_moment: float32 [2048, 2048], P(('shard', 'context'), 'tensor'), may hold values from -640 to 640
- out_moment: float32 [2048, 2048], P('tensor', ('shard', 'context')), may hold values from -256 to 256
- gate_moment: float32 [2048, 8192], P(('shard', 'context'), 'tensor'), may hold values from -192 to 192
- up_moment: float32 [2048, 8192], P(('shard', 'context'), 'tensor'), may hold values from -192 to 192
- down_moment: float32 [8192, 2048], P('tensor', ('shard', 'context')), may hold values from -384 to 384
- query_average: float32 [2048, 2048], P(('shard', 'context'), 'tensor'), may hold values from -0.1875 to 0.1875
- key_average: float32 [2048, 2048], P(('shard', 'context'), 'tensor'), may hold values from -0.1875 to 0.1875
- value_average: float32 [2048, 2048], P(('shard', 'context'), 'tensor'), may hold values from -0.125 to 0.125
- out_average: float32 [2048, 2048], P('tensor', ('shard', 'context')), may hold values from -0.5 to 0.5
- gate_average: float32 [2048, 8192], P(('shard', 'context'), 'tensor'), may hold values from -0.125 to 0.125
- up_average: float32 [2048, 8192], P(('shard', 'context'), 'tensor'), may hold values from -0.125 to 0.125
- down_average: float32 [8192, 2048], P('tensor', ('shard', 'context')), may hold values from -0.0625 to 0.0625
Outputs:
- block_output: bfloat16 [4, 4, 2, 256, 2048], P('shard', None, 'context')
- input_grad: bfloat16 [4, 4, 2, 256, 2048], P(None, 'shard', 'context')
- query_gradient: float32 [2048, 2048], P(('shard', 'context'), 'tensor')
- key_gradient: float32 [2048, 2048], P(('shard', 'context'), 'tensor')
- value_gradient: float32 [2048, 2048], P(('shard', 'context'), 'tensor')
- out_gradient: float32 [2048, 2048], P('tensor', ('shard', 'context'))
- gate_gradient: float32 [2048, 8192], P(('shard', 'context'), 'tensor')
- up_gradient: float32 [2048, 8192], P(('shard', 'context'), 'tensor')
- down_gradient: float32 [8192, 2048], P('tensor', ('shard', 'context'))
- query_momentum: float32 [2048, 2048], P(('shard', 'context'), 'tensor')
- key_momentum: float32 [2048, 2048], P(('shard', 'context'), 'tensor')
- value_momentum: float32 [2048, 2048], P(('shard', 'context'), 'tensor')
- out_momentum: float32 [2048, 2048], P('tensor', ('shard', 'context'))
- gate_momentum: float32 [2048, 8192], P(('shard', 'context'), 'tensor')
- up_momentum: float32 [2048, 8192], P(('shard', 'context'), 'tensor')
- down_momentum: float32 [8192, 2048], P('tensor', ('shard', 'context'))
- query_master: float32 [2048, 2048], P(('shard', 'context'), 'tensor')
- key_master: float32 [2048, 2048], P(('shard', 'context'), 'tensor')
- value_master: float32 [2048, 2048], P(('shard', 'context'), 'tensor')
- out_master: float32 [2048, 2048], P('tensor', ('shard', 'context'))
- gate_master: float32 [2048, 8192], P(('shard', 'context'), 'tensor')
- up_master: float32 [2048, 8192], P(('shard', 'context'), 'tensor')
- down_master: float32 [8192, 2048], P('tensor', ('shard', 'context'))
- query_mean: float32 [2048, 2048], P(('shard', 'context'), 'tensor')
- key_mean: float32 [2048, 2048], P(('shard', 'context'), 'tensor')
- value_mean: float32 [2048, 2048], P(('shard', 'context'), 'tensor')
- out_mean: float32 [2048, 2048], P('tensor', ('shard', 'context'))
- gate_mean: float32 [2048, 8192], P(('shard', 'context'), 'tensor')
- up_mean: float32 [2048, 8192], P(('shard', 'context'), 'tensor')
- down_mean: float32 [8192, 2048], P('tensor', ('shard', 'context'))
The draws below stay inside these ranges and needn't reach their ends.
Inputs may be any that keep to these rules, and one draw needn't show every extreme that they name: lengths gives each sequence's tokens by data index; the longest is exactly 2048. order holds each data index once.
All inputs are finite; a program needn't handle non-finite values.
Results may differ from the reference program's by a relative error of at most 0.015.
The reference program's roundings to bfloat16 on the way count: a program that leaves them out, or rounds other values in their place, can miss the bound.
Values may be sent and summed in bfloat16 or wider, within the bound.
A program may use at most 384 MiB of HBM per device.

```python
import jax
import jax.numpy as jnp
from jax import lax

D = 2048
HD = 128
FF = 8192
LSLOT = 2048
LMIN = 1024
SEQS = 4
STRIPE = 256
N_SHARD = 4
N_CONTEXT = 2


def draw_lengths(key, part):
    first_key, second_key = jax.random.split(jax.random.fold_in(key, 17))
    values = jax.random.randint(first_key, (SEQS,), LMIN, LSLOT + 1, dtype=jnp.int32)
    chosen = jax.random.randint(second_key, (), 0, SEQS, dtype=jnp.int32)
    return jnp.where(jnp.arange(SEQS, dtype=jnp.int32) == chosen, LSLOT, values).astype(jnp.int32)


def level_of(rng, shape, cuts, least, high):
    factor_of, own = 1.0, jax.random.fold_in(rng, 6)
    for position, shards_of in cuts:
        steps = jnp.exp(jax.random.uniform(jax.random.fold_in(own, position), (shards_of,), jnp.float32, least / len(cuts), high / len(cuts)))
        factor_of = factor_of * jnp.repeat(steps, shape[position] // shards_of).reshape([-1 if axis == position else 1 for axis in range(len(shape))])
    return factor_of


def centred(own_key, dims, scale, limit, cuts=(), kind=jnp.bfloat16):
    array = jax.random.normal(own_key, dims, jnp.float32) * scale
    if len(cuts) > 0:
        array = level_of(own_key, dims, cuts, -0.22, 0.18) * array
    return jnp.clip(array, min=-limit, max=limit).astype(kind)


def setup_inputs(seed: int = 0) -> dict:
    splits = jax.random.split(jax.random.key(seed), 26)
    return {
        "x_data": centred(splits[0], (SEQS, N_SHARD, N_CONTEXT, STRIPE, D), 1.0, 6.0, ((1, 4), (2, 2))),
        "cotangent": centred(splits[1], (SEQS, N_SHARD, N_CONTEXT, STRIPE, D), 1.0, 6.0, ((0, 4), (2, 2))),
        "lengths": draw_lengths(jax.random.fold_in(splits[25], 71), 0),
        "order": jax.random.permutation(splits[3], SEQS).astype(jnp.int32),
        "query_weight": centred(splits[4], (D, D), (D // 2) ** -0.5, 0.1875, ((0, 8), (1, 4)), jnp.float32),
        "key_weight": centred(splits[5], (D, D), (D // 2) ** -0.5, 0.1875, ((0, 8), (1, 4)), jnp.float32),
        "value_weight": centred(splits[6], (D, D), D ** -0.5, 0.125, ((0, 8), (1, 4)), jnp.float32),
        "out_weight": centred(splits[7], (D, D), (D // 16) ** -0.5, 0.5, ((0, 4), (1, 8)), jnp.float32),
        "gate_weight": centred(splits[8], (D, FF), D ** -0.5, 0.125, ((0, 8), (1, 4)), jnp.float32),
        "up_weight": centred(splits[9], (D, FF), D ** -0.5, 0.125, ((0, 8), (1, 4)), jnp.float32),
        "down_weight": centred(splits[10], (FF, D), FF ** -0.5, 0.0625, ((0, 4), (1, 8)), jnp.float32),
        "query_moment": centred(splits[11], (D, D), 150.0, 896.0, ((0, 8), (1, 4)), jnp.float32),
        "key_moment": centred(splits[12], (D, D), 150.0, 896.0, ((0, 8), (1, 4)), jnp.float32),
        "value_moment": centred(splits[13], (D, D), 100.0, 640.0, ((0, 8), (1, 4)), jnp.float32),
        "out_moment": centred(splits[14], (D, D), 40.0, 256.0, ((0, 4), (1, 8)), jnp.float32),
        "gate_moment": centred(splits[15], (D, FF), 30.0, 192.0, ((0, 8), (1, 4)), jnp.float32),
        "up_moment": centred(splits[16], (D, FF), 30.0, 192.0, ((0, 8), (1, 4)), jnp.float32),
        "down_moment": centred(splits[17], (FF, D), 60.0, 384.0, ((0, 4), (1, 8)), jnp.float32),
        "query_average": centred(splits[18], (D, D), ((D // 2) ** -0.5), 0.1875, ((0, 8), (1, 4)), jnp.float32),
        "key_average": centred(splits[19], (D, D), ((D // 2) ** -0.5), 0.1875, ((0, 8), (1, 4)), jnp.float32),
        "value_average": centred(splits[20], (D, D), (D ** -0.5), 0.125, ((0, 8), (1, 4)), jnp.float32),
        "out_average": centred(splits[21], (D, D), ((D // 16) ** -0.5), 0.5, ((0, 4), (1, 8)), jnp.float32),
        "gate_average": centred(splits[22], (D, FF), (D ** -0.5), 0.125, ((0, 8), (1, 4)), jnp.float32),
        "up_average": centred(splits[23], (D, FF), (D ** -0.5), 0.125, ((0, 8), (1, 4)), jnp.float32),
        "down_average": centred(splits[24], (FF, D), (FF ** -0.5), 0.0625, ((0, 4), (1, 8)), jnp.float32),
    }


@jax.custom_vjp
def low(v):
    return lax.optimization_barrier(v.astype(jnp.bfloat16)).astype(jnp.float32)

@jax.custom_vjp
def low_back(v):
    return v

def low_keep(v):
    return (low(v), None)

def low_pass(kept, grad):
    return (grad,)

def back_keep(v):
    return (v, None)

def back_low(kept, grad):
    return (low(grad),)
low.defvjp(low_keep, low_pass)
low_back.defvjp(back_keep, back_low)
norm_epsilon = 1e-05
momentum_coef = 0.9
average_decay = 0.9
learn_rate = 0.0001
rope_base = 10000.0
masked_score = -1e+30
highest = lax.Precision.HIGHEST

def layer_norm(values):
    center = lax.optimization_barrier(jnp.mean(values, axis=-1, keepdims=True))
    shifted = values - center
    spread = lax.optimization_barrier(jnp.mean(shifted * shifted, axis=-1, keepdims=True))
    return shifted * lax.rsqrt(spread + norm_epsilon)

def rotate_heads(values, positions, direction):
    half_size = values.shape[-1] // 2
    inverse_freq = rope_base ** (-(jnp.arange(half_size, dtype=jnp.float32) * 2.0 / values.shape[-1]))
    angles = positions.astype(jnp.float32)[:, None] * inverse_freq[None, :]
    cosine = jnp.cos(angles)[:, None, :]
    sine_part = direction * jnp.sin(angles)[:, None, :]
    first_half = values[..., :half_size]
    second = values[..., half_size:]
    return jnp.concatenate([first_half * cosine - second * sine_part, second * cosine + first_half * sine_part], axis=-1)

def matmul_high(left, right):
    return jnp.dot(left, right, preferred_element_type=jnp.float32, precision=highest)

def attend_reference(query_block, block_pos, key_rot, value_heads, key_pos, seq_length):
    score_scale = HD ** (-0.5)
    scores = low_back(jnp.einsum('qhd,khd->hqk', query_block, key_rot, precision=highest)) * score_scale
    allowed = (key_pos[None, :] <= block_pos[:, None]) & (key_pos[None, :] < seq_length)
    scaled = jnp.where(allowed[None], scores, masked_score)
    top_score = lax.optimization_barrier(jnp.max(scaled, axis=-1, keepdims=True))
    exp_terms = jnp.exp(scaled - top_score)
    totals = lax.optimization_barrier(jnp.sum(exp_terms, axis=-1, keepdims=True))
    attn_probs = low(exp_terms / totals)
    return jnp.einsum('hqk,khd->qhd', attn_probs, value_heads, precision=highest)

def sequence_forward(inputs, seq_length, query_weight, key_weight, value_weight, out_weight, gate_weight, up_weight, down_weight):
    length_rows = inputs.shape[0]
    heads_count = inputs.shape[1] // HD
    positions = jnp.arange(length_rows, dtype=jnp.int32)
    normed_one = low(layer_norm(inputs))
    query_lin = low_back(matmul_high(normed_one, low(query_weight))).reshape(length_rows, heads_count, HD)
    key_lin = low_back(matmul_high(normed_one, low(key_weight))).reshape(length_rows, heads_count, HD)
    query_rot = low_back(low(rotate_heads(query_lin, positions, 1.0)))
    key_rot = low_back(low(rotate_heads(key_lin, positions, 1.0)))
    value_heads = low_back(low(matmul_high(normed_one, low(value_weight)))).reshape(length_rows, heads_count, HD)
    block_rows = min(512, length_rows)
    block_count = length_rows // block_rows
    query_blocks = query_rot.reshape(block_count, block_rows, heads_count, HD)
    pos_blocks = positions.reshape(block_count, block_rows)

    def one_block(pieces):
        return attend_reference(pieces[0], pieces[1], key_rot, value_heads, positions, seq_length)
    attended = lax.map(jax.checkpoint(one_block), (query_blocks, pos_blocks))
    attn_heads = low_back(low(attended.reshape(length_rows, heads_count * HD)))
    hidden = inputs + low_back(matmul_high(attn_heads, low(out_weight)))
    normed_two = low(layer_norm(hidden))
    gate_act = low_back(matmul_high(normed_two, low(gate_weight)))
    up_act = low_back(matmul_high(normed_two, low(up_weight)))
    swish = low(gate_act * jax.nn.sigmoid(gate_act) * up_act)
    return hidden + low_back(matmul_high(swish, low(down_weight)))

def nesterov(master, moment, average, gradient):
    momentum = momentum_coef * moment + gradient
    updated = master - learn_rate * (gradient + momentum_coef * momentum)
    mean_new = average_decay * average + (1.0 - average_decay) * updated
    return (momentum, updated, mean_new)

def reference(x_data, cotangent, lengths, order, query_weight, key_weight, value_weight, out_weight, gate_weight, up_weight, down_weight, query_moment, key_moment, value_moment, out_moment, gate_moment, up_moment, down_moment, query_average, key_average, value_average, out_average, gate_average, up_average, down_average):
    masters = (query_weight, key_weight, value_weight, out_weight, gate_weight, up_weight, down_weight)
    moments = (query_moment, key_moment, value_moment, out_moment, gate_moment, up_moment, down_moment)
    averages = (query_average, key_average, value_average, out_average, gate_average, up_average, down_average)
    slot_count = x_data.shape[0]
    seq_len = x_data.shape[1] * x_data.shape[2] * x_data.shape[3]
    model_width = x_data.shape[4]
    inputs_all = x_data.astype(jnp.float32).reshape(slot_count, seq_len, model_width)
    cot_all = cotangent.astype(jnp.float32).reshape(slot_count, seq_len, model_width)

    def one_slot(running, slot_index):
        source = order[slot_index]
        seq_length = lengths[source]
        inputs = inputs_all[source]
        valid_rows = (jnp.arange(seq_len, dtype=jnp.int32) < seq_length).astype(jnp.float32)[:, None]

        def forward_fn(values, *weights):
            return sequence_forward(values, seq_length, *weights)
        output, pullback = jax.vjp(forward_fn, inputs, *masters)
        gradients = pullback(cot_all[slot_index] * valid_rows)
        updated = tuple((total + grad_piece for total, grad_piece in zip(running, gradients[1:])))
        return (updated, (output.astype(jnp.bfloat16), gradients[0].astype(jnp.bfloat16)))
    start_totals = tuple((jnp.zeros_like(master) for master in masters))
    totals, (outputs, slot_grads) = lax.scan(one_slot, start_totals, jnp.arange(slot_count, dtype=jnp.int32))
    block_output = outputs.reshape(cotangent.shape)
    input_grad = jnp.zeros((slot_count, seq_len, model_width), jnp.bfloat16).at[order].set(slot_grads).reshape(x_data.shape)
    states = [nesterov(masters[item], moments[item], averages[item], totals[item]) for item in range(7)]
    return (block_output, input_grad, totals[0], totals[1], totals[2], totals[3], totals[4], totals[5], totals[6], states[0][0], states[1][0], states[2][0], states[3][0], states[4][0], states[5][0], states[6][0], states[0][1], states[1][1], states[2][1], states[3][1], states[4][1], states[5][1], states[6][1], states[0][2], states[1][2], states[2][2], states[3][2], states[4][2], states[5][2], states[6][2])
```

```python
import functools

import jax
import jax.numpy as jnp
from jax import lax
from jax.experimental import pallas as pl
from jax.experimental.pallas import tpu as pltpu
from jax.sharding import PartitionSpec as P

HD = 128
CORES = 2

norm_epsilon = 1e-05
momentum_coef = 0.9
average_decay = 0.9
learn_rate = 0.0001
rope_base = 10000.0
masked_score = -1e30

f32 = jnp.float32
bf16 = jnp.bfloat16
PLANE = ("context", "tensor")


def after(value, *deps):
    return lax.optimization_barrier((value,) + deps)[0]


def layer_norm_rows(values):
    center = jnp.mean(values, axis=-1, keepdims=True)
    shifted = values - center
    spread = jnp.mean(shifted * shifted, axis=-1, keepdims=True)
    inverse = lax.rsqrt(spread + norm_epsilon)
    return (shifted * inverse, inverse)


def norm_backward(upstream, normed, inverse):
    mean_grad = jnp.mean(upstream, axis=-1, keepdims=True)
    mean_proj = jnp.mean(upstream * normed, axis=-1, keepdims=True)
    return inverse * (upstream - mean_grad - normed * mean_proj)


def matmul(left, right):
    return jnp.dot(left, right, preferred_element_type=f32)


def matmul_tn(left, right):
    return lax.dot_general(left, right, (((0,), (0,)), ((), ())), preferred_element_type=f32)


def matmul_nt(left, right):
    return lax.dot_general(left, right, (((1,), (1,)), ((), ())), preferred_element_type=f32)


def plane_shift(value, dx, dy, swap):
    nc, nt = lax.axis_size("context"), lax.axis_size("tensor")
    ny = nt // CORES
    pairs = []
    for x in range(nc):
        for y in range(ny):
            for core in range(CORES):
                target = ((x + dx) % nc) * nt + ((y + dy) % ny) * CORES + (core ^ swap)
                pairs.append((x * nt + y * CORES + core, target))
    return lax.ppermute(value, PLANE, pairs)


def plane_shifts():
    nc, ny = lax.axis_size("context"), lax.axis_size("tensor") // CORES
    return [(dx, dy) for dx in range(nc) for dy in range(ny)]


def plane_place():
    nc, nt = lax.axis_size("context"), lax.axis_size("tensor")
    t = lax.axis_index("tensor")
    return lax.axis_index("context"), t // CORES, t % CORES, nc, nt // CORES


def put(buffer, piece, *where):
    shape = (piece.shape[0],) + (1,) * len(where) + piece.shape[1:]
    return lax.dynamic_update_slice(buffer, piece.reshape(shape), (0,) + where + (0, 0))


def plane_gather(block):
    x, y, core, nc, ny = plane_place()
    rows, inner, width = block.shape
    buffer = jnp.zeros((rows, nc, ny * CORES, inner, width), block.dtype)
    for dx, dy in plane_shifts():
        piece = block if dx == 0 and dy == 0 else plane_shift(block, dx, dy, 0)
        other = plane_shift(piece, 0, 0, 1)
        px, py = (x - dx) % nc, (y - dy) % ny
        buffer = put(buffer, piece, px, py * CORES + core)
        buffer = put(buffer, other, px, py * CORES + 1 - core)
    return buffer


def tensor_gather(block):
    x, y, core, nc, ny = plane_place()
    rows, inner, width = block.shape
    buffer = jnp.zeros((rows, ny * CORES, inner, width), block.dtype)
    for dy in range(ny):
        piece = block if dy == 0 else plane_shift(block, 0, dy, 0)
        other = plane_shift(piece, 0, 0, 1)
        py = (y - dy) % ny
        buffer = put(buffer, piece, py * CORES + core)
        buffer = put(buffer, other, py * CORES + 1 - core)
    return buffer


def plane_reduce(partial):
    x, y, core, nc, ny = plane_place()
    rows, _, _, inner, width = partial.shape

    def piece(px, py, pc):
        got = lax.dynamic_slice(
            partial, (0, px, py * CORES + pc, 0, 0), (rows, 1, 1, inner, width)
        )
        return got.reshape(rows, inner, width)

    total = None
    arrived = []
    for dx, dy in reversed(plane_shifts()):
        px, py = (x + dx) % nc, (y + dy) % ny
        other = plane_shift(piece(px, py, 1 - core), 0, 0, 1)
        chip = piece(px, py, core).astype(f32) + other.astype(f32)
        if dx == 0 and dy == 0:
            total = chip
        else:
            arrived.append(plane_shift(chip.astype(bf16), dx, dy, 0))
    for value in arrived:
        total = total + value.astype(f32)
    return total


def line_gather(block, gates):
    ns = lax.axis_size("shard")
    z = lax.axis_index("shard")
    up = after(block, gates[0]) if gates else block
    down = after(block, gates[1]) if gates else block
    ups, downs = [None], [None]
    for step in range(1, ns):
        up = lax.ppermute(up, "shard", [(i, i + 1) for i in range(step - 1, ns - 1)])
        down = lax.ppermute(down, "shard", [(i, i - 1) for i in range(1, ns - step + 1)])
        ups.append(up)
        downs.append(down)
    buffer = jnp.zeros((ns,) + block.shape, block.dtype)
    buffer = lax.dynamic_update_slice(buffer, block[None], (z, 0, 0))
    for step in range(1, ns):
        piece = jnp.where(z >= step, ups[step], downs[ns - step])
        buffer = lax.dynamic_update_slice(buffer, piece[None], ((z - step) % ns, 0, 0))
    late = max(1, ns - 2)
    return buffer, (ups[late], downs[late])


def line_reduce(partial, gates):
    ns = lax.axis_size("shard")
    z = lax.axis_index("shard")

    def slab(index):
        return lax.dynamic_index_in_dim(partial, index % ns, 0, keepdims=False)

    up, down = slab(z + ns - 1), slab(z + 1)
    if gates:
        up, down = after(up, gates[0]), after(down, gates[1])
    ups, downs = [None], [None]
    for step in range(1, ns):
        if step > 1:
            up = (slab(z + ns - step).astype(f32) + up.astype(f32)).astype(bf16)
            down = (slab(z - ns + step).astype(f32) + down.astype(f32)).astype(bf16)
        up = lax.ppermute(up, "shard", [(i, i + 1) for i in range(step)])
        down = lax.ppermute(down, "shard", [(i, i - 1) for i in range(ns - step, ns)])
        ups.append(up)
        downs.append(down)
    late = max(1, ns - 2)
    own = slab(z).astype(f32) + up.astype(f32) + down.astype(f32)
    return own, (ups[late], downs[late])


def attend_forward_body(scale, bq, len_ref, q_ref, k_ref, v_ref, o_ref, lse_ref):
    i = pl.program_id(1)
    length = len_ref[0]
    q = q_ref[...]
    q_pos = i * bq + lax.broadcasted_iota(jnp.int32, (1, bq), 1)
    limit = jnp.minimum(q_pos, length - 1)
    row = lax.broadcasted_iota(jnp.int32, (bq, bq), 0)

    def step(j, carry):
        top, total, acc = carry
        keys = pl.ds(pl.multiple_of(j * bq, bq), bq)
        s = matmul_nt(k_ref[keys, :], q) * scale
        s = jnp.where(row <= limit - j * bq, s, masked_score)
        new_top = jnp.maximum(top, jnp.max(s, axis=0, keepdims=True))
        p = jnp.exp(s - new_top)
        shrink = jnp.exp(top - new_top)
        total = total * shrink + jnp.sum(p, axis=0, keepdims=True)
        acc = acc * shrink + matmul_tn(v_ref[keys, :], p.astype(bf16))
        return new_top, total, acc

    start = (
        jnp.full((1, bq), masked_score, f32),
        jnp.zeros((1, bq), f32),
        jnp.zeros((HD, bq), f32),
    )
    top, total, acc = lax.fori_loop(0, i + 1, step, start)
    o_ref[...] = jnp.transpose(acc / total).astype(bf16)
    lse_ref[0] = top + jnp.log(total)


def attend_forward(qkv, length, heads, bq):
    rows = qkv.shape[0]
    grid = (heads, rows // bq)
    return pl.pallas_call(
        functools.partial(attend_forward_body, HD ** (-0.5), bq),
        out_shape=(
            jax.ShapeDtypeStruct((rows, heads * HD), bf16),
            jax.ShapeDtypeStruct((heads, 1, rows), f32),
        ),
        grid_spec=pltpu.PrefetchScalarGridSpec(
            num_scalar_prefetch=1,
            grid=grid,
            in_specs=[
                pl.BlockSpec((bq, HD), lambda h, i, n: (i, h)),
                pl.BlockSpec((rows, HD), lambda h, i, n: (0, heads + h)),
                pl.BlockSpec((rows, HD), lambda h, i, n: (0, 2 * heads + h)),
            ],
            out_specs=(
                pl.BlockSpec((bq, HD), lambda h, i, n: (i, h)),
                pl.BlockSpec((1, 1, bq), lambda h, i, n: (h, 0, i)),
            ),
        ),
        cost_estimate=pl.CostEstimate(
            flops=heads * rows * rows * HD * 2 * 3,
            bytes_accessed=rows * heads * HD * 8,
            transcendentals=heads * rows * rows,
        ),
        name="attend_forward",
    )(length, qkv, qkv, qkv)


def attend_backward_body(
    scale, bq, len_ref, q_ref, k_ref, v_ref, lse_ref, g_ref, dq_ref, dk_ref, dv_ref,
    p_scr, dp_scr, dk_acc, dv_acc,
):
    i = pl.program_id(1)
    length = len_ref[0]
    q = q_ref[...]
    g = g_ref[...]
    lse = lse_ref[0]
    q_pos = i * bq + lax.broadcasted_iota(jnp.int32, (1, bq), 1)
    limit = jnp.minimum(q_pos, length - 1)
    row = lax.broadcasted_iota(jnp.int32, (bq, bq), 0)

    @pl.when(i == 0)
    def _():
        dk_acc[...] = jnp.zeros_like(dk_acc)
        dv_acc[...] = jnp.zeros_like(dv_acc)

    def first(j, dot):
        keys = pl.ds(pl.multiple_of(j * bq, bq), bq)
        s = matmul_nt(k_ref[keys, :], q) * scale
        p = jnp.where(row <= limit - j * bq, jnp.exp(s - lse), 0.0)
        dp = matmul_nt(v_ref[keys, :], g)
        dv_acc[keys, :] += matmul(p.astype(bf16), g)
        p_scr[keys, :] = p
        dp_scr[keys, :] = dp
        return dot + jnp.sum(p * dp, axis=0, keepdims=True)

    dot = lax.fori_loop(0, i + 1, first, jnp.zeros((1, bq), f32))

    def second(j, acc):
        keys = pl.ds(pl.multiple_of(j * bq, bq), bq)
        ds = (p_scr[keys, :] * (dp_scr[keys, :] - dot) * scale).astype(bf16)
        dk_acc[keys, :] += matmul(ds, q)
        return acc + matmul_tn(k_ref[keys, :], ds)

    acc = lax.fori_loop(0, i + 1, second, jnp.zeros((HD, bq), f32))
    dq_ref[...] = jnp.transpose(acc).astype(bf16)

    @pl.when(i == pl.num_programs(1) - 1)
    def _():
        dk_ref[...] = dk_acc[...].astype(bf16)
        dv_ref[...] = dv_acc[...].astype(bf16)


def attend_backward(qkv, length, lse, grad, heads, bq):
    rows = qkv.shape[0]
    grid = (heads, rows // bq)
    out = jax.ShapeDtypeStruct((rows, heads * HD), bf16)
    return pl.pallas_call(
        functools.partial(attend_backward_body, HD ** (-0.5), bq),
        out_shape=(out, out, out),
        grid_spec=pltpu.PrefetchScalarGridSpec(
            num_scalar_prefetch=1,
            grid=grid,
            in_specs=[
                pl.BlockSpec((bq, HD), lambda h, i, n: (i, h)),
                pl.BlockSpec((rows, HD), lambda h, i, n: (0, heads + h)),
                pl.BlockSpec((rows, HD), lambda h, i, n: (0, 2 * heads + h)),
                pl.BlockSpec((1, 1, bq), lambda h, i, n: (h, 0, i)),
                pl.BlockSpec((bq, HD), lambda h, i, n: (i, h)),
            ],
            out_specs=(
                pl.BlockSpec((bq, HD), lambda h, i, n: (i, h)),
                pl.BlockSpec((rows, HD), lambda h, i, n: (0, h)),
                pl.BlockSpec((rows, HD), lambda h, i, n: (0, h)),
            ),
            scratch_shapes=[
                pltpu.VMEM((rows, bq), f32),
                pltpu.VMEM((rows, bq), f32),
                pltpu.VMEM((rows, HD), f32),
                pltpu.VMEM((rows, HD), f32),
            ],
        ),
        cost_estimate=pl.CostEstimate(
            flops=heads * rows * rows * HD * 2 * 6,
            bytes_accessed=rows * heads * HD * 16,
            transcendentals=heads * rows * rows,
        ),
        name="attend_backward",
    )(length, qkv, qkv, qkv, lse, grad)


def rotate(values, cosine, sine):
    rows = values.shape[0]
    heads = values.reshape(rows, -1, HD)
    half = HD // 2
    turned = jnp.concatenate([heads[..., half:], heads[..., :half]], axis=-1)
    return (heads * cosine[:, None, :] + turned * sine[:, None, :]).reshape(values.shape)


def nesterov(master, moment, average, gradient):
    momentum = momentum_coef * moment + gradient
    updated = master - learn_rate * (gradient + momentum_coef * momentum)
    mean_new = average_decay * average + (1.0 - average_decay) * updated
    return (momentum, updated, mean_new)


def local(x_data, cotangent, lengths, order, *params):
    masters, moments, averages = params[:7], params[7:14], params[14:]
    ns, nc, nt = lax.axis_size("shard"), lax.axis_size("context"), lax.axis_size("tensor")
    z, x, t = lax.axis_index("shard"), lax.axis_index("context"), lax.axis_index("tensor")
    seqs, _, _, stripe, width = x_data.shape
    part = stripe // nt
    total_rows = ns * nc * stripe
    my_length = lengths[order[z]]
    length_arg = my_length.reshape(1)

    own_x = jnp.zeros((ns, part, width), bf16)
    for step in range(ns):
        seq = order[(z + step) % ns]
        piece = lax.dynamic_slice(x_data, (seq, 0, 0, t * part, 0), (1, 1, 1, part, width))
        piece = piece.reshape(1, part, width)
        if step:
            piece = lax.ppermute(piece, "shard", [(i, (i + step) % ns) for i in range(ns)])
        own_x = lax.dynamic_update_slice(own_x, piece, ((z - step) % ns, 0, 0))

    def halves(pieces):
        mine, theirs = [], []
        for block in pieces:
            split = block.astype(bf16).reshape(block.shape[0], nc, block.shape[1] // nc)
            mine.append(lax.dynamic_index_in_dim(split, x, 1, keepdims=False))
            theirs.append(lax.dynamic_index_in_dim(split, (x + 1) % nc, 1, keepdims=False))
        return jnp.concatenate(mine, axis=1), jnp.concatenate(theirs, axis=1)

    def slab(pieces):
        mine, theirs = halves(pieces)
        got = lax.ppermute(theirs, "context", [(i, (i + 1) % nc) for i in range(nc)])
        first = jnp.where(x == 0, mine, got)
        second = jnp.where(x == 0, got, mine)
        return jnp.concatenate([first, second], axis=0)

    group_pieces = (
        (masters[0], masters[1], masters[2]),
        (masters[3].T,),
        (masters[4],),
        (masters[5],),
        (masters[6].T,),
    )
    gates = ()
    full = []
    for pieces in group_pieces:
        gathered, gates = line_gather(slab(pieces), gates)
        full.append(gathered.reshape(width, gathered.shape[-1]))
    w_qkv, w_out, w_gate, w_up, w_down = full
    heads = w_out.shape[1] // HD

    position = jnp.arange(total_rows, dtype=jnp.int32)
    half = HD // 2
    inverse_freq = rope_base ** (-(jnp.arange(half, dtype=f32) * 2.0 / HD))
    angles = position.astype(f32)[:, None] * inverse_freq[None, :]
    cosine = jnp.concatenate([jnp.cos(angles)] * 2, axis=-1)
    sine_half = jnp.sin(angles)
    sine = jnp.concatenate([-sine_half, sine_half], axis=-1)

    input_rows = own_x.astype(f32)
    normed_one, inverse_one = layer_norm_rows(input_rows)
    attn_input = plane_gather(normed_one.astype(bf16)).reshape(total_rows, width)
    qkv_lin = matmul(attn_input, w_qkv)
    qk = rotate(qkv_lin[:, : 2 * heads * HD], cosine, sine).astype(bf16)
    qkv = jnp.concatenate([qk, qkv_lin[:, 2 * heads * HD :].astype(bf16)], axis=1)
    bq = min(512, total_rows)
    attn_heads, lse = attend_forward(qkv, length_arg, heads, bq)
    plane_shape = (ns, nc, nt, part, width)
    attn_part = matmul_nt(attn_heads, w_out).astype(bf16).reshape(plane_shape)
    hidden = input_rows + plane_reduce(attn_part)
    normed_two, inverse_two = layer_norm_rows(hidden)

    row_in = jnp.arange(ns * stripe, dtype=jnp.int32)
    own_pos = (row_in // stripe * nc + x) * stripe + row_in % stripe
    valid = (own_pos < my_length).reshape(1, ns, 1, stripe, 1)
    loss_own = jnp.where(valid, cotangent, jnp.zeros_like(cotangent)).reshape(
        ns, nt, part, width
    )
    loss_rows = lax.dynamic_index_in_dim(loss_own, t, 1, keepdims=False)
    _, y, core, _, ny = plane_place()
    loss_grad = jnp.zeros(plane_shape, bf16)
    loss_grad = lax.dynamic_update_slice(loss_grad, loss_own[:, None], (0, x, 0, 0, 0))
    for dx in range(1, nc):
        across = plane_shift(loss_rows, dx, 0, 0)
        px = (x - dx) % nc
        for dy in range(ny):
            piece = plane_shift(across, 0, dy, 0) if dy else across
            other = plane_shift(piece, 0, 0, 1)
            py = (y - dy) % ny
            loss_grad = put(loss_grad, piece, px, py * CORES + core)
            loss_grad = put(loss_grad, other, px, py * CORES + 1 - core)
    loss_grad = loss_grad.reshape(total_rows, width)

    ffn_input = plane_gather(normed_two.astype(bf16)).reshape(total_rows, width)
    gate_act = matmul(ffn_input, w_gate)
    up_act = matmul(ffn_input, w_up)
    sigmoid_gate = jax.nn.sigmoid(gate_act)
    swish = (gate_act * sigmoid_gate * up_act).astype(bf16)
    down_wgrad = matmul_tn(loss_grad, swish).astype(bf16)
    swish_grad = matmul(loss_grad, w_down)
    gate_grad = (
        swish_grad * up_act * sigmoid_gate * (1.0 + gate_act * (1.0 - sigmoid_gate))
    ).astype(bf16)
    up_grad = (swish_grad * gate_act * sigmoid_gate).astype(bf16)
    back_part = matmul_nt(gate_grad, w_gate) + matmul_nt(up_grad, w_up)
    ffn_in_grad = plane_reduce(back_part.astype(bf16).reshape(plane_shape))
    ffn_part = matmul_nt(swish, w_down).astype(bf16).reshape(plane_shape)
    gate_wgrad = matmul_tn(ffn_input, gate_grad).astype(bf16)
    up_wgrad = matmul_tn(ffn_input, up_grad).astype(bf16)

    hidden_grad = loss_rows.astype(f32) + norm_backward(ffn_in_grad, normed_two, inverse_two)
    attn_out_grad = plane_gather(hidden_grad.astype(bf16)).reshape(total_rows, width)
    out_wgrad = matmul_tn(attn_out_grad, attn_heads).astype(bf16)
    heads_grad = matmul(attn_out_grad, w_out).astype(bf16)
    dq, dk, dv = attend_backward(qkv, length_arg, lse, heads_grad, heads, bq)
    dqk = rotate(jnp.concatenate([dq, dk], axis=1).astype(f32), cosine, -sine).astype(bf16)
    dqkv = jnp.concatenate([dqk, dv], axis=1)
    input_part = matmul_nt(dqkv, w_qkv).astype(bf16).reshape(plane_shape)
    norm_in_grad = plane_reduce(input_part)
    qkv_wgrad = matmul_tn(attn_input, dqkv).astype(bf16)
    input_grad_own = (hidden_grad + norm_backward(norm_in_grad, normed_one, inverse_one)).astype(
        bf16
    )

    returned = jnp.zeros((seqs, part, width), bf16)
    for step in range(ns):
        piece = lax.dynamic_slice_in_dim(input_grad_own, (z + step) % ns, 1, 0)
        if step:
            piece = lax.ppermute(piece, "shard", [(i, (i + step) % ns) for i in range(ns)])
        returned = lax.dynamic_update_slice(returned, piece, (order[(z - step) % ns], 0, 0))
    input_grad = tensor_gather(returned).reshape(x_data.shape)

    output_rows = (hidden + plane_reduce(ffn_part)).astype(bf16)
    block_output = tensor_gather(output_rows).reshape(cotangent.shape)

    gates = ()
    owned = []
    for grad in (down_wgrad, gate_wgrad, up_wgrad, out_wgrad, qkv_wgrad):
        own, gates = line_reduce(grad.reshape(ns, width // ns, grad.shape[1]), gates)
        own = own.reshape(nc, width // ns // nc, grad.shape[1])
        keep = lax.dynamic_index_in_dim(own, x, 0, keepdims=False)
        send = lax.dynamic_index_in_dim(own, (x + 1) % nc, 0, keepdims=False).astype(bf16)
        got = lax.ppermute(send, "context", [(i, (i + 1) % nc) for i in range(nc)]).astype(f32)
        owned.append((keep, got))

    def whole(keep, got):
        first = jnp.where(x == 0, keep, got)
        second = jnp.where(x == 0, got, keep)
        return jnp.concatenate([first, second], axis=1)

    span = heads * HD
    down_pair, gate_pair, up_pair, out_pair, qkv_pair = owned
    wgrads = [
        whole(qkv_pair[0][:, n * span : (n + 1) * span], qkv_pair[1][:, n * span : (n + 1) * span])
        for n in range(3)
    ]
    wgrads.append(whole(*out_pair).T)
    wgrads.append(whole(*gate_pair))
    wgrads.append(whole(*up_pair))
    wgrads.append(whole(*down_pair).T)
    states = [
        nesterov(masters[item], moments[item], averages[item], wgrads[item]) for item in range(7)
    ]
    return (
        (block_output, input_grad)
        + tuple(wgrads)
        + tuple(state[0] for state in states)
        + tuple(state[1] for state in states)
        + tuple(state[2] for state in states)
    )


def solution(mesh):
    rows = P(("shard", "context"), "tensor")
    cols = P("tensor", ("shard", "context"))
    weights = (rows, rows, rows, cols, rows, rows, cols)
    data = P(None, "shard", "context", None, None)
    work = P("shard", None, "context", None, None)
    return jax.shard_map(
        local,
        mesh=mesh,
        in_specs=(data, work, P(), P()) + weights * 3,
        out_specs=(work, data) + weights * 4,
        check_vma=False,
    )
```

```python
import functools

import jax
import jax.numpy as jnp
from jax import lax
from jax.experimental import pallas as pl
from jax.experimental.pallas import tpu as pltpu
from jax.sharding import PartitionSpec as P


HD = 128
CORES = 2

norm_epsilon = 1e-05
momentum_coef = 0.9
average_decay = 0.9
learn_rate = 0.0001
rope_base = 10000.0
masked_score = -1e30

f32 = jnp.float32
bf16 = jnp.bfloat16
SHD, CTX, TEN = "shard", "context", "tensor"
PLANE = (CTX, TEN)


def after(value, *deps):
    return lax.optimization_barrier((value,) + deps)[0]


def layer_norm_rows(values):
    center = jnp.mean(values, axis=-1, keepdims=True)
    shifted = values - center
    spread = jnp.mean(shifted * shifted, axis=-1, keepdims=True)
    inverse = lax.rsqrt(spread + norm_epsilon)
    return (shifted * inverse, inverse)


def norm_backward(upstream, normed, inverse):
    mean_grad = jnp.mean(upstream, axis=-1, keepdims=True)
    mean_proj = jnp.mean(upstream * normed, axis=-1, keepdims=True)
    return inverse * (upstream - mean_grad - normed * mean_proj)


def matmul(left, right):
    return jnp.dot(left, right, preferred_element_type=f32)


def matmul_tn(left, right):
    return lax.dot_general(left, right, (((0,), (0,)), ((), ())), preferred_element_type=f32)


def matmul_nt(left, right):
    return lax.dot_general(left, right, (((1,), (1,)), ((), ())), preferred_element_type=f32)


def blank(shape, dtype):
    return pl.pallas_call(
        lambda out: None,
        out_shape=jax.ShapeDtypeStruct(shape, dtype),
        out_specs=pl.BlockSpec(memory_space=pl.ANY),
        cost_estimate=pl.CostEstimate(flops=0, bytes_accessed=0, transcendentals=0),
    )()


def plane_shift(value, dx, dy, swap):
    nc, nt = lax.axis_size(CTX), lax.axis_size(TEN)
    ny = nt // CORES
    pairs = []
    for x in range(nc):
        for y in range(ny):
            for core in range(CORES):
                target = ((x + dx) % nc) * nt + ((y + dy) % ny) * CORES + (core ^ swap)
                pairs.append((x * nt + y * CORES + core, target))
    return lax.ppermute(value, PLANE, pairs)


def plane_shifts():
    nc, ny = lax.axis_size(CTX), lax.axis_size(TEN) // CORES
    return [(dx, dy) for dx in range(nc) for dy in range(ny)]


def plane_place():
    nc, nt = lax.axis_size(CTX), lax.axis_size(TEN)
    t = lax.axis_index(TEN)
    return lax.axis_index(CTX), t // CORES, t % CORES, nc, nt // CORES


def put(buffer, piece, *where, row=0):
    shape = (piece.shape[0],) + (1,) * len(where) + piece.shape[1:]
    return lax.dynamic_update_slice(buffer, piece.reshape(shape), (0,) + where + (row, 0))


def plane_gather(blocks):
    x, y, core, nc, ny = plane_place()
    rows, inner, width = blocks[0].shape
    buffer = blank((rows, nc, ny * CORES, inner * len(blocks), width), blocks[0].dtype)
    for order, block in enumerate(blocks):
        pieces = []
        for dx, dy in plane_shifts():
            pieces.append(plane_shift(block, dx, dy, 0) if dx or dy else block)
        for (dx, dy), piece in zip(plane_shifts(), pieces):
            other = plane_shift(piece, 0, 0, 1)
            px, py = (x - dx) % nc, (y - dy) % ny
            buffer = put(buffer, piece, px, py * CORES + core, row=order * inner)
            buffer = put(buffer, other, px, py * CORES + 1 - core, row=order * inner)
    return buffer


def tensor_gather(block, buffer, row=0):
    _, y, core, _, ny = plane_place()
    for dy in range(ny):
        piece = plane_shift(block, 0, dy, 0) if dy else block
        other = plane_shift(piece, 0, 0, 1)
        py = (y - dy) % ny
        buffer = put(buffer, piece, py * CORES + core, row=row)
        buffer = put(buffer, other, py * CORES + 1 - core, row=row)
    return buffer


def plane_reduce(partial, parts=1):
    x, y, core, nc, ny = plane_place()
    rows, _, _, inner, width = partial.shape
    inner = inner // parts

    def piece(px, py, pc, order):
        got = lax.dynamic_slice(
            source,
            (0, px, py * CORES + pc, order * inner, 0),
            (rows, 1, 1, inner, width),
        )
        return got.reshape(rows, inner, width)

    source = partial
    kept, sent, arrived = [], [], []
    for order in range(parts):
        if order:
            source = after(source, *sent)
        for dx, dy in reversed(plane_shifts()):
            px, py = (x + dx) % nc, (y + dy) % ny
            other = plane_shift(piece(px, py, 1 - core, order), 0, 0, 1)
            chip = piece(px, py, core, order).astype(f32) + other.astype(f32)
            if dx == 0 and dy == 0:
                kept.append(chip)
            else:
                sent.append(chip.astype(bf16))
                arrived.append(plane_shift(sent[-1], dx, dy, 0))
    each = len(arrived) // parts
    totals = []
    for order in range(parts):
        total = kept[order]
        mine = arrived[order * each : (order + 1) * each]
        if order + 1 < parts:
            mine, _ = lax.optimization_barrier((mine, sent))
        for value in mine:
            total = total + value.astype(f32)
        totals.append(total)
    return totals


def cut(value, parts):
    return jnp.split(value, parts, axis=1)


def line_gather(block):
    return lax.all_gather(block, SHD, axis=0, tiled=True)


def line_reduce(partial):
    return lax.psum_scatter(partial, SHD, scatter_dimension=0, tiled=True)


def turn(values, cosine, sine):
    return values * cosine + pltpu.roll(values, HD // 2, 1) * sine


def attend_forward_body(
    scale, bq, len_ref, q_ref, k_ref, v_ref, cos_ref, sin_ref,
    o_ref, lse_ref, qr_ref, kr_ref, vr_ref,
):
    i = pl.program_id(1)
    length = len_ref[0]
    mine = pl.ds(pl.multiple_of(i * bq, bq), bq)
    q = turn(q_ref[...], cos_ref[mine, :], sin_ref[mine, :]).astype(bf16)
    qr_ref[...] = q
    kr_ref[mine, :] = turn(k_ref[...], cos_ref[mine, :], sin_ref[mine, :]).astype(bf16)
    vr_ref[mine, :] = v_ref[...].astype(bf16)
    q_pos = i * bq + lax.broadcasted_iota(jnp.int32, (1, bq), 1)
    limit = jnp.minimum(q_pos, length - 1)
    row = lax.broadcasted_iota(jnp.int32, (bq, bq), 0)

    def step(j, carry):
        top, total, acc = carry
        keys = pl.ds(pl.multiple_of(j * bq, bq), bq)
        s = matmul_nt(kr_ref[keys, :], q) * scale
        s = jnp.where(row <= limit - j * bq, s, masked_score)
        new_top = jnp.maximum(top, jnp.max(s, axis=0, keepdims=True))
        p = jnp.exp(s - new_top)
        shrink = jnp.exp(top - new_top)
        total = total * shrink + jnp.sum(p, axis=0, keepdims=True)
        acc = acc * shrink + matmul_tn(vr_ref[keys, :], p.astype(bf16))
        return new_top, total, acc

    start = (
        jnp.full((1, bq), masked_score, f32),
        jnp.zeros((1, bq), f32),
        jnp.zeros((HD, bq), f32),
    )
    top, total, acc = lax.fori_loop(0, i + 1, step, start)
    o_ref[...] = jnp.transpose(acc / total).astype(bf16)
    lse_ref[0] = top + jnp.log(total)


def attend_forward(qkv, cosine, sine, length, heads, bq):
    rows = qkv.shape[0]
    out = jax.ShapeDtypeStruct((rows, heads * HD), bf16)
    block = pl.BlockSpec((bq, HD), lambda h, i, n: (i, h))
    whole = pl.BlockSpec((rows, HD), lambda h, i, n: (0, h))
    table = pl.BlockSpec((rows, HD), lambda h, i, n: (0, 0))
    return pl.pallas_call(
        functools.partial(attend_forward_body, HD ** (-0.5), bq),
        out_shape=(out, jax.ShapeDtypeStruct((heads, 1, rows), f32), out, out, out),
        grid_spec=pltpu.PrefetchScalarGridSpec(
            num_scalar_prefetch=1,
            grid=(heads, rows // bq),
            in_specs=[
                block,
                pl.BlockSpec((bq, HD), lambda h, i, n: (i, heads + h)),
                pl.BlockSpec((bq, HD), lambda h, i, n: (i, 2 * heads + h)),
                table,
                table,
            ],
            out_specs=(
                block,
                pl.BlockSpec((1, 1, bq), lambda h, i, n: (h, 0, i)),
                block,
                whole,
                whole,
            ),
        ),
        cost_estimate=pl.CostEstimate(
            flops=heads * rows * rows * HD * 2 * 3,
            bytes_accessed=rows * heads * HD * 24,
            transcendentals=heads * rows * rows,
        ),
        name="af",
    )(length, qkv, qkv, qkv, cosine, sine)


def attend_backward_body(
    scale, bq, len_ref, q_ref, k_ref, v_ref, lse_ref, g_ref, cos_ref, sin_ref,
    dq_ref, dk_ref, dv_ref, p_scr, dp_scr, dk_acc, dv_acc,
):
    i = pl.program_id(1)
    length = len_ref[0]
    q = q_ref[...]
    g = g_ref[...]
    lse = lse_ref[0]
    q_pos = i * bq + lax.broadcasted_iota(jnp.int32, (1, bq), 1)
    limit = jnp.minimum(q_pos, length - 1)
    row = lax.broadcasted_iota(jnp.int32, (bq, bq), 0)

    @pl.when(i == 0)
    def _():
        dk_acc[...] = jnp.zeros_like(dk_acc)
        dv_acc[...] = jnp.zeros_like(dv_acc)

    def first(j, dot):
        keys = pl.ds(pl.multiple_of(j * bq, bq), bq)
        s = matmul_nt(k_ref[keys, :], q) * scale
        p = jnp.where(row <= limit - j * bq, jnp.exp(s - lse), 0.0)
        dp = matmul_nt(v_ref[keys, :], g)
        dv_acc[keys, :] += matmul(p.astype(bf16), g)
        p_scr[keys, :] = p
        dp_scr[keys, :] = dp
        return dot + jnp.sum(p * dp, axis=0, keepdims=True)

    dot = lax.fori_loop(0, i + 1, first, jnp.zeros((1, bq), f32))

    def second(j, acc):
        keys = pl.ds(pl.multiple_of(j * bq, bq), bq)
        ds = (p_scr[keys, :] * (dp_scr[keys, :] - dot) * scale).astype(bf16)
        dk_acc[keys, :] += matmul(ds, q)
        return acc + matmul_tn(k_ref[keys, :], ds)

    acc = lax.fori_loop(0, i + 1, second, jnp.zeros((HD, bq), f32))
    mine = pl.ds(pl.multiple_of(i * bq, bq), bq)
    dq = jnp.transpose(acc).astype(bf16).astype(f32)
    dq_ref[...] = turn(dq, cos_ref[mine, :], -sin_ref[mine, :]).astype(bf16)

    @pl.when(i == pl.num_programs(1) - 1)
    def _():
        dk = dk_acc[...].astype(bf16).astype(f32)
        dk_ref[...] = turn(dk, cos_ref[...], -sin_ref[...]).astype(bf16)
        dv_ref[...] = dv_acc[...].astype(bf16)


def attend_backward(q, k, v, cosine, sine, length, lse, grad, heads, bq):
    rows = q.shape[0]
    out = jax.ShapeDtypeStruct((rows, heads * HD), bf16)
    block = pl.BlockSpec((bq, HD), lambda h, i, n: (i, h))
    whole = pl.BlockSpec((rows, HD), lambda h, i, n: (0, h))
    table = pl.BlockSpec((rows, HD), lambda h, i, n: (0, 0))
    return pl.pallas_call(
        functools.partial(attend_backward_body, HD ** (-0.5), bq),
        out_shape=(out, out, out),
        grid_spec=pltpu.PrefetchScalarGridSpec(
            num_scalar_prefetch=1,
            grid=(heads, rows // bq),
            in_specs=[
                block,
                whole,
                whole,
                pl.BlockSpec((1, 1, bq), lambda h, i, n: (h, 0, i)),
                block,
                table,
                table,
            ],
            out_specs=(block, whole, whole),
            scratch_shapes=[
                pltpu.VMEM((rows, bq), f32),
                pltpu.VMEM((rows, bq), f32),
                pltpu.VMEM((rows, HD), f32),
                pltpu.VMEM((rows, HD), f32),
            ],
        ),
        cost_estimate=pl.CostEstimate(
            flops=heads * rows * rows * HD * 2 * 6,
            bytes_accessed=rows * heads * HD * 16,
            transcendentals=heads * rows * rows,
        ),
        name="ab",
    )(length, q, k, v, lse, grad, cosine, sine)


def nesterov_body(
    turned, x_ref, kept_ref, got_ref, master_ref, moment_ref, average_ref,
    gradient_out, momentum_out, master_out, mean_out,
):
    mine = pl.program_id(0) == x_ref[0]
    gradient = jnp.where(mine, kept_ref[...].astype(f32), got_ref[...].astype(f32))
    if turned:
        gradient = jnp.transpose(gradient)
    momentum = momentum_coef * moment_ref[...] + gradient
    updated = master_ref[...] - learn_rate * (gradient + momentum_coef * momentum)
    gradient_out[...] = gradient
    momentum_out[...] = momentum
    master_out[...] = updated
    mean_out[...] = average_decay * average_ref[...] + (1.0 - average_decay) * updated


def nesterov(kept, got, column, place, master, moment, average, turned):
    nc = lax.axis_size(CTX)
    rows = got.shape[0]
    span = master.shape[0 if turned else 1] // nc
    tile = min(span, 512)
    per = span // tile
    if turned:
        block = pl.BlockSpec((tile, rows), lambda h, c, n: (h * per + c, 0))
    else:
        block = pl.BlockSpec((rows, tile), lambda h, c, n: (0, h * per + c))
    out = jax.ShapeDtypeStruct(master.shape, f32)
    return pl.pallas_call(
        functools.partial(nesterov_body, turned),
        out_shape=(out,) * 4,
        grid_spec=pltpu.PrefetchScalarGridSpec(
            num_scalar_prefetch=1,
            grid=(nc, per),
            in_specs=[
                pl.BlockSpec((rows, tile), lambda h, c, n: (n[0], column * per + c)),
                pl.BlockSpec((rows, tile), lambda h, c, n: (0, column * per + c)),
                block,
                block,
                block,
            ],
            out_specs=(block,) * 4,
        ),
        cost_estimate=pl.CostEstimate(
            flops=master.size * 8, bytes_accessed=master.size * 32, transcendentals=0
        ),
        name="nu",
    )(place, kept, got, master, moment, average)


def local(x_data, cotangent, lengths, order, *params):
    masters, moments, averages = params[:7], params[7:14], params[14:]
    ns, nc, nt = lax.axis_size(SHD), lax.axis_size(CTX), lax.axis_size(TEN)
    z, x, t = lax.axis_index(SHD), lax.axis_index(CTX), lax.axis_index(TEN)
    seqs, _, _, stripe, width = x_data.shape
    part = stripe // nt
    total_rows = ns * nc * stripe
    my_length = lengths[order[z]]
    length_arg = my_length.reshape(1)

    own_x = blank((ns, part, width), bf16)
    for step in range(ns):
        seq = order[(z + step) % ns]
        piece = lax.dynamic_slice(x_data, (seq, 0, 0, t * part, 0), (1, 1, 1, part, width))
        piece = piece.reshape(1, part, width)
        if step:
            piece = lax.ppermute(piece, SHD, [(i, (i + step) % ns) for i in range(ns)])
        own_x = lax.dynamic_update_slice(own_x, piece, ((z - step) % ns, 0, 0))

    def halves(pieces):
        mine, theirs = [], []
        for block in pieces:
            split = block.astype(bf16).reshape(block.shape[0], nc, block.shape[1] // nc)
            mine.append(lax.dynamic_index_in_dim(split, x, 1, keepdims=False))
            theirs.append(lax.dynamic_index_in_dim(split, (x + 1) % nc, 1, keepdims=False))
        return jnp.concatenate(mine, axis=1), jnp.concatenate(theirs, axis=1)

    def slab(pieces):
        mine, theirs = halves(pieces)
        got = lax.ppermute(theirs, CTX, [(i, (i + 1) % nc) for i in range(nc)])
        first = jnp.where(x == 0, mine, got)
        second = jnp.where(x == 0, got, mine)
        return jnp.concatenate([first, second], axis=0)

    group_pieces = (
        (masters[0], masters[1], masters[2]),
        (masters[3].T,),
        (masters[4],),
        (masters[5],),
        (masters[6].T,),
    )
    full = []
    for pieces in group_pieces:
        ready = slab(pieces)
        full.append(line_gather(ready))
    w_qkv, w_out, w_gate, w_up, w_down = full
    heads = w_out.shape[1] // HD

    position = jnp.arange(total_rows, dtype=jnp.int32)
    half = HD // 2
    inverse_freq = rope_base ** (-(jnp.arange(half, dtype=f32) * 2.0 / HD))
    angles = position.astype(f32)[:, None] * inverse_freq[None, :]
    cosine = jnp.concatenate([jnp.cos(angles)] * 2, axis=-1)
    sine_half = jnp.sin(angles)
    sine = jnp.concatenate([-sine_half, sine_half], axis=-1)

    input_rows = own_x.astype(f32)
    normed_one, inverse_one = layer_norm_rows(input_rows)
    attn_input = plane_gather([normed_one.astype(bf16)]).reshape(total_rows, width)
    qkv_lin = matmul(attn_input, w_qkv)
    bq = min(512, total_rows)
    attn_heads, lse, q_rot, k_rot, v_heads = attend_forward(
        qkv_lin, cosine, sine, length_arg, heads, bq
    )
    plane_shape = (ns, nc, nt, part, width)
    attn_part = matmul_nt(attn_heads, w_out).astype(bf16).reshape(plane_shape)
    hidden = input_rows + plane_reduce(attn_part)[0]
    normed_two, inverse_two = layer_norm_rows(hidden)

    row_in = jnp.arange(ns * stripe, dtype=jnp.int32)
    own_pos = (row_in // stripe * nc + x) * stripe + row_in % stripe
    valid = (own_pos < my_length).reshape(1, ns, 1, stripe, 1)
    loss_own = jnp.where(valid, cotangent, jnp.zeros_like(cotangent)).reshape(ns, nt, part, width)
    row_pos = own_pos.reshape(ns, nt, part)
    row_pos = lax.dynamic_index_in_dim(row_pos, t, 1, keepdims=False)
    loss_rows = lax.dynamic_slice(
        cotangent, (0, 0, 0, t * part, 0), (1, ns, 1, part, width)
    ).reshape(ns, part, width)
    loss_rows = jnp.where(
        (row_pos < my_length)[:, :, None], loss_rows, jnp.zeros_like(loss_rows)
    )
    _, y, core, _, ny = plane_place()
    loss_grad = blank(plane_shape, bf16)
    loss_grad = lax.dynamic_update_slice(loss_grad, loss_own[:, None], (0, x, 0, 0, 0))
    for dx in range(1, nc):
        across = plane_shift(loss_rows, dx, 0, 0)
        px = (x - dx) % nc
        for dy in range(ny):
            piece = plane_shift(across, 0, dy, 0) if dy else across
            other = plane_shift(piece, 0, 0, 1)
            py = (y - dy) % ny
            loss_grad = put(loss_grad, piece, px, py * CORES + core)
            loss_grad = put(loss_grad, other, px, py * CORES + 1 - core)
    loss_grad = loss_grad.reshape(total_rows, width)

    ffn_input = plane_gather([normed_two.astype(bf16)]).reshape(total_rows, width)
    gate_act = matmul(ffn_input, w_gate)
    up_act = matmul(ffn_input, w_up)
    sigmoid_gate = jax.nn.sigmoid(gate_act)
    swish = (gate_act * sigmoid_gate * up_act).astype(bf16)
    w_down = after(w_down, swish)
    down_wgrad = matmul_tn(loss_grad, swish).astype(bf16)
    swish_grad = matmul(loss_grad, w_down)
    gate_grad = (
        swish_grad * up_act * sigmoid_gate * (1.0 + gate_act * (1.0 - sigmoid_gate))
    ).astype(bf16)
    up_grad = (swish_grad * gate_act * sigmoid_gate).astype(bf16)
    back_part = matmul_nt(gate_grad, w_gate) + matmul_nt(up_grad, w_up)
    parts = 2
    ffn_in_grads = plane_reduce(back_part.astype(bf16).reshape(plane_shape), parts)
    ffn_part = matmul_nt(swish, w_down).astype(bf16).reshape(plane_shape)
    gate_wgrad = matmul_tn(ffn_input, gate_grad).astype(bf16)
    up_wgrad = matmul_tn(ffn_input, up_grad).astype(bf16)

    hidden_grads = []
    for rows, grad, normed, inverse in zip(
        cut(loss_rows, parts), ffn_in_grads, cut(normed_two, parts), cut(inverse_two, parts)
    ):
        if hidden_grads:
            grad = after(grad, hidden_grads[-1])
        hidden_grads.append(rows.astype(f32) + norm_backward(grad, normed, inverse))
    attn_out_grad = plane_gather([grad.astype(bf16) for grad in hidden_grads])
    attn_out_grad = attn_out_grad.reshape(total_rows, width)
    out_wgrad = matmul_tn(attn_out_grad, attn_heads).astype(bf16)
    heads_grad = matmul(attn_out_grad, w_out).astype(bf16)
    dq, dk, dv = attend_backward(
        q_rot, k_rot, v_heads, cosine, sine, length_arg, lse, heads_grad, heads, bq
    )
    dqkv = jnp.concatenate([dq, dk, dv], axis=1)
    input_part = matmul_nt(dqkv, w_qkv).astype(bf16).reshape(plane_shape)
    norm_in_grads = plane_reduce(input_part, parts)
    qkv_wgrad = matmul_tn(attn_input, dqkv).astype(bf16)
    input_grad = blank((seqs, nt, part, width), bf16)
    each = part // parts
    for cut_order, (hidden_grad, grad, normed, inverse) in enumerate(
        zip(hidden_grads, norm_in_grads, cut(normed_one, parts), cut(inverse_one, parts))
    ):
        if cut_order:
            grad = after(grad, own_grad)
        own_grad = (hidden_grad + norm_backward(grad, normed, inverse)).astype(bf16)
        returned = blank((seqs, each, width), bf16)
        for step in range(ns):
            piece = lax.dynamic_slice_in_dim(own_grad, (z + step) % ns, 1, 0)
            if step:
                piece = lax.ppermute(piece, SHD, [(i, (i + step) % ns) for i in range(ns)])
            returned = lax.dynamic_update_slice(
                returned, piece, (order[(z - step) % ns], 0, 0)
            )
        input_grad = tensor_gather(returned, input_grad, cut_order * each)
    input_grad = input_grad.reshape(x_data.shape)

    output_rows = (hidden + plane_reduce(ffn_part)[0]).astype(bf16)
    block_output = tensor_gather(output_rows, blank((ns, nt, part, width), bf16))
    block_output = block_output.reshape(cotangent.shape)

    owned = []
    for grad in (down_wgrad, gate_wgrad, up_wgrad, out_wgrad, qkv_wgrad):
        own = line_reduce(grad)
        size = own.shape[0] // nc
        send = lax.dynamic_slice_in_dim(own, (x + 1) % nc * size, size, 0)
        got = lax.ppermute(send, CTX, [(i, (i + 1) % nc) for i in range(nc)])
        owned.append((own, got))

    down_pair, gate_pair, up_pair, out_pair, qkv_pair = owned
    sources = (
        (qkv_pair, 0),
        (qkv_pair, 1),
        (qkv_pair, 2),
        (out_pair, 0),
        (gate_pair, 0),
        (up_pair, 0),
        (down_pair, 0),
    )
    states = []
    for item, name in enumerate("qkvogud"):
        (kept, got), column = sources[item]
        states.append(
            nesterov(
                kept, got, column, x.reshape(1), masters[item], moments[item],
                averages[item], name in "od",
            )
        )
    return (
        (block_output, input_grad)
        + tuple(state[0] for state in states)
        + tuple(state[1] for state in states)
        + tuple(state[2] for state in states)
        + tuple(state[3] for state in states)
    )


def solution(mesh):
    rows = P((SHD, CTX), TEN)
    cols = P(TEN, (SHD, CTX))
    weights = (rows, rows, rows, cols, rows, rows, cols)
    data = P(None, SHD, CTX, None, None)
    work = P(SHD, None, CTX, None, None)
    return jax.shard_map(
        local,
        mesh=mesh,
        in_specs=(data, work, P(), P()) + weights * 3,
        out_specs=(work, data) + weights * 4,
        check_vma=False,
    )
```
